8 devices in a mesh: fsdp: 8 (over z, y, x, core).
Axes of the slice: x: 2, y: 2, z: 1, core: 2. Of those that a mesh axis runs over, the one named last changes fastest.
Arguments:
- x: bfloat16 [2, 16384, 2048], P(None, 'fsdp')
- g: bfloat16 [2, 16384, 2048], P(None, 'fsdp')
- w1: bfloat16 [1, 2048, 8192], P(None, 'fsdp')
- w2: bfloat16 [1, 8192, 2048], P(None, 'fsdp')
Outputs:
- output 1: bfloat16 [2, 16384, 2048], P(None, 'fsdp')
- output 2: float32 [1, 2048, 8192], P(None, 'fsdp')
- output 3: float32 [1, 8192, 2048], P(None, 'fsdp')
All inputs are finite; a program needn't handle non-finite values.
Results may differ from the reference program's by a relative error of at most 0.001.
Values are sent between devices in bfloat16 or wider.
A program may use at most 1 GiB of HBM per device.

```python
import jax
import jax.numpy as jnp
from jax import lax

D = 2048
FF = 8192
LAYERS = 1
MICRO = 2
TOKENS = 16384


def setup_inputs(seed: int = 0) -> dict:
    k1, k2, k3, k4 = jax.random.split(jax.random.key(seed), 4)
    w1 = jax.random.normal(k1, (LAYERS, D, FF), jnp.float32) * D ** -0.5
    w2 = jax.random.normal(k2, (LAYERS, FF, D), jnp.float32) * FF ** -0.5
    x = jax.random.normal(k3, (MICRO, TOKENS, D), jnp.float32)
    g = jax.random.normal(k4, (MICRO, TOKENS, D), jnp.float32) * (MICRO * TOKENS) ** -0.5
    return {"x": x.astype(jnp.bfloat16), "g": g.astype(jnp.bfloat16),
            "w1": w1.astype(jnp.bfloat16), "w2": w2.astype(jnp.bfloat16)}


def _gelu_bwd(a, e):
    return jax.vjp(jax.nn.gelu, a)[1](e)[0]


def _micro(w1, w2, x, g):
    def fwd(xl, ws):
        v1, v2 = ws
        a = jnp.dot(xl, v1, preferred_element_type=jnp.float32).astype(jnp.bfloat16)
        h = jax.nn.gelu(a.astype(jnp.float32)).astype(jnp.bfloat16)
        y = (xl.astype(jnp.float32) + jnp.dot(h, v2, preferred_element_type=jnp.float32)).astype(jnp.bfloat16)
        return y, (xl, a)

    y, (xs, acts) = lax.scan(fwd, x, (w1, w2))

    def bwd(gy, inp):
        v1, v2, xl, a = inp
        h = jax.nn.gelu(a.astype(jnp.float32)).astype(jnp.bfloat16)
        e = jnp.dot(gy, v2.T, preferred_element_type=jnp.float32)
        da = _gelu_bwd(a.astype(jnp.float32), e).astype(jnp.bfloat16)
        dw2 = jnp.dot(h.T, gy, preferred_element_type=jnp.float32)
        dw1 = jnp.dot(xl.T, da, preferred_element_type=jnp.float32)
        gx = (gy.astype(jnp.float32) + jnp.dot(da, v1.T, preferred_element_type=jnp.float32)).astype(jnp.bfloat16)
        return gx, (dw1, dw2)

    _, (dw1, dw2) = lax.scan(bwd, g, (w1, w2, xs, acts), reverse=True)
    return y, dw1, dw2


def reference(x, g, w1, w2):
    def step(acc, xg):
        y, dw1, dw2 = _micro(w1, w2, xg[0], xg[1])
        return (acc[0] + dw1, acc[1] + dw2), y

    zeros = (jnp.zeros(w1.shape, jnp.float32), jnp.zeros(w2.shape, jnp.float32))
    (dw1, dw2), y = lax.scan(step, zeros, (x, g))
    return (y, dw1, dw2)
```

```python
import functools

import jax
import jax.numpy as jnp
from jax import lax
from jax.experimental import pallas as pl
from jax.experimental.pallas import tpu as pltpu
from jax.sharding import PartitionSpec as P

AX = "fsdp"
F32 = jnp.float32
BF16 = jnp.bfloat16
MESH = pl.DeviceIdType.MESH
C0 = 0.7978845608028654
C1 = 0.044715
D = 2048
HF = 4096
TOK = 4096
T = 2 * TOK
B = 1024
SUB = 256
VMEM = 60 * 2**20


def _gelu(a):
    return a * (0.5 * (1.0 + jnp.tanh(C0 * (a + C1 * (a * a * a)))))


def _gelu_grad(a):
    a2 = a * a
    t = jnp.tanh(C0 * (a + C1 * (a2 * a)))
    return 0.5 * (1.0 + t) + (0.5 * a) * (1.0 - t * t) * (C0 + (3.0 * C1 * C0) * a2)


def _kernel(x, g, w1, w2,
            y, dw2, o1, o1r, r1f, xa, ga, w1g, w2g, aa, ha, da, s2, r2, s1, r1, yp, yr,
            xs, xr, w1s, w1r, w2s, w2r, s2s, s2r, s1s, s1r, os, orr, ys, yrs):
    me = lax.axis_index(AX)
    c, q = me % 2, me // 2
    qx, qy = q % 2, q // 2
    nx, ny, nd = 2 * qy + (1 - qx), 2 * (1 - qy) + qx, 3 - q
    dev = lambda chip, core: 2 * chip + core
    peer = dev(q, 1 - c)

    def blk(i):
        return 2 * ((qy + i // 2) % 2) + (qx + i % 2) % 2

    def rdma(src, dst, ss, rs, to):
        return pltpu.make_async_remote_copy(src_ref=src, dst_ref=dst, send_sem=ss, recv_sem=rs,
                                            device_id=(to,), device_id_type=MESH)

    cx = rdma(x, xa.at[pl.ds(TOK, TOK)], xs.at[0], xr.at[0], peer)
    cg = rdma(g, ga.at[pl.ds(TOK, TOK)], xs.at[1], xr.at[1], peer)

    def w1_rows(owner, j):
        return w1g.at[pl.ds(owner * 256, 256), pl.ds(j * B, B)]

    def w1_out(j):
        def one(role, rsem, p, to):
            return rdma(w1.at[:, pl.ds((2 * j + p) * B, B)], w1_rows(me, j), w1s.at[j, role], w1r.at[j, rsem], to)
        return [one(1, 1 + c, 0, dev(nx, 0)), one(2, 1 + c, 1, dev(nx, 1)),
                one(3, 3 + c, 0, dev(ny, 0)), one(4, 3 + c, 1, dev(ny, 1)),
                one(0, 0, 1 - c, peer)]

    def w1_in(j):
        def one(owner, rsem):
            return rdma(w1_rows(owner, j), w1_rows(owner, j), w1s.at[j, 0], w1r.at[j, rsem], peer)
        return [one(peer, 0), one(dev(nx, 0), 1), one(dev(nx, 1), 2), one(dev(ny, 0), 3), one(dev(ny, 1), 4)]

    def w1_relay(j):
        ra, rb = w1_rows(dev(nx, 0), j), w1_rows(dev(ny, 1), j)
        return [rdma(ra, ra, w1s.at[j, 5], w1r.at[j, 5], dev(ny, c)),
                rdma(rb, rb, w1s.at[j, 6], w1r.at[j, 6], dev(nx, c))]

    def w1_relay_in(j):
        ra, rb = w1_rows(dev(nd, 0), j), w1_rows(dev(nd, 1), j)
        return [rdma(ra, ra, w1s.at[j, 5], w1r.at[j, 5], peer), rdma(rb, rb, w1s.at[j, 6], w1r.at[j, 6], peer)]

    def w2_rows(chip, lo, n):
        return w2g.at[pl.ds(chip * B + lo, n)]

    w2_out = [rdma(w2, w2_rows(q, 0, B), w2s.at[0], w2r.at[0], dev(nx, c)),
              rdma(w2, w2_rows(q, 0, B), w2s.at[1], w2r.at[1], dev(ny, c))]
    w2_in = [rdma(w2_rows(nx, 0, B), w2_rows(nx, 0, B), w2s.at[0], w2r.at[0], peer),
             rdma(w2_rows(ny, 0, B), w2_rows(ny, 0, B), w2s.at[1], w2r.at[1], peer)]
    w2_relay = [rdma(w2_rows(nx, 0, B // 2), w2_rows(nx, 0, B // 2), w2s.at[2], w2r.at[2], dev(ny, c)),
                rdma(w2_rows(ny, B // 2, B // 2), w2_rows(ny, B // 2, B // 2), w2s.at[3], w2r.at[3], dev(nx, c))]
    w2_relay_in = [rdma(w2_rows(nd, 0, B // 2), w2_rows(nd, 0, B // 2), w2s.at[2], w2r.at[2], peer),
                   rdma(w2_rows(nd, B // 2, B // 2), w2_rows(nd, B // 2, B // 2), w2s.at[3], w2r.at[3], peer)]

    p2 = [rdma(s2.at[k], r2.at[k], s2s.at[k], s2r.at[k], dev(nx if k in (0, 2, 4) else ny, c)) for k in range(6)]
    p1d = [rdma(s1.at[k], r1.at[k], s1s.at[k, 0], s1r.at[k, 0], dev(nx if k == 0 else ny, c)) for k in range(2)]
    p1 = [[rdma(s1.at[k, pl.ds(256 * p, 256)], r1f.at[k - 2, c], s1s.at[k, p], s1r.at[k, c], dev(nx if k in (2, 4) else ny, p))
           for p in range(2)] for k in range(2, 6)]
    p1_in = [[rdma(s1.at[k, pl.ds(256 * p, 256)], r1f.at[k - 2, p], s1s.at[k, p], s1r.at[k, p], peer)
              for p in range(2)] for k in range(2, 6)]
    co = rdma(o1.at[:, pl.ds(256 * (1 - c), 256)], o1r, os.at[0], orr.at[0], peer)
    cy = rdma(yp, yr, ys.at[0], yrs.at[0], peer)

    def copy_body(*refs):
        n = len(refs) // 2
        for i in range(n):
            refs[n + i][...] = refs[i][...]

    def a_phase(j):
        def body(x_ref, w_ref, a_ref, h_ref):
            @pl.when((pl.program_id(0) == 6) & (j < 3))
            def _():
                for d in w1_in(j + 1):
                    d.wait_recv()
                for d in w1_relay(j + 1):
                    d.start()

            @pl.when((pl.program_id(0) == 6) & (j < 2))
            def _():
                for d in w1_out(j + 2):
                    d.start()

            @pl.when((pl.program_id(0) == 6) & (j == 2))
            def _():
                for d in w2_out:
                    d.start()

            for n in range(B // SUB):
                s = slice(n * SUB, (n + 1) * SUB)
                a = jnp.dot(x_ref[...], w_ref[:, s], preferred_element_type=F32).astype(BF16)
                a_ref[:, s] = a
                h_ref[:, s] = _gelu(a.astype(F32)).astype(BF16)

        out = pl.BlockSpec((B, B), lambda i: (i, j))
        pltpu.emit_pipeline(body, grid=(T // B,),
                            in_specs=[pl.BlockSpec((B, D), lambda i: (i, 0)), pl.BlockSpec((D, B), lambda i: (0, j))],
                            out_specs=[out, out])(xa, w1g, aa, ha)

    def e_phase(lo, n):
        def body(g_ref, w_ref, a_ref, d_ref):
            for m in range(B // SUB):
                s = slice(m * SUB, (m + 1) * SUB)
                e = lax.dot_general(g_ref[...], w_ref[s, :], (((1,), (1,)), ((), ())), preferred_element_type=F32)
                d_ref[:, s] = (_gelu_grad(a_ref[:, s].astype(F32)) * e).astype(BF16)

        act = pl.BlockSpec((B, B), lambda i, k: (k, blk(i + lo)))
        pltpu.emit_pipeline(body, grid=(n, T // B),
                            in_specs=[pl.BlockSpec((B, D), lambda i, k: (k, 0)),
                                      pl.BlockSpec((B, D), lambda i, k: (blk(i + lo), 0)), act],
                            out_specs=[act])(ga, w2g, aa, da)

    def tn(lhs, rhs, out, m, n, li, ri, out_spec, recv=()):
        def body(l_ref, r_ref, *rest):
            o_ref = rest[-1]
            @pl.when(pl.program_id(1) == 0)
            def _():
                init = jnp.zeros(o_ref.shape, F32)
                for r in rest[:-1]:
                    init = init + r[...].reshape(o_ref.shape)
                o_ref[...] = init
            o_ref[...] += lax.dot_general(l_ref[...], r_ref[...], (((0,), (0,)), ((), ())),
                                          preferred_element_type=F32).reshape(o_ref.shape)

        pltpu.emit_pipeline(body, grid=(2, T // B),
                            in_specs=[pl.BlockSpec((B, m), lambda i, k: (k, li(i))), pl.BlockSpec((B, n), lambda i, k: (k, ri(i)))]
                            + [pl.BlockSpec((1, m, n), functools.partial(lambda f, i, k: (f(i), 0, 0), f)) for _, f in recv],
                            out_specs=[out_spec])(lhs, rhs, *[r for r, _ in recv], out)

    half = pl.BlockSpec((1, B, B), lambda i, k: (i, 0, 0))
    half1 = pl.BlockSpec((1, 512, D), lambda i, k: (i, 0, 0))
    near = lambda i: (1 - i) * nx + i * ny
    d2 = lambda slot, li, ri, recv=(): tn(ha, ga, s2.at[pl.ds(slot, 2)], B, B, li, ri, half, recv)
    d1 = lambda slot, li, ri, recv=(): tn(xa, da, s1.at[pl.ds(slot, 2)], 512, D, li, ri, half1, recv)

    def y_phase(own):
        def body(h_ref, w_ref, *rest):
            v = jnp.dot(h_ref[...], w_ref[...], preferred_element_type=F32)
            if own:
                x_ref, r_ref, o_ref = rest
                o_ref[...] = (x_ref[...].astype(F32) + (v + r_ref[...])).astype(BF16)
            else:
                rest[0][...] = v

        bm = 512
        base = 0 if own else TOK // bm
        col = pl.BlockSpec((bm, B), lambda n, i: (i, n))
        pltpu.emit_pipeline(body, grid=(2, TOK // bm),
                            in_specs=[pl.BlockSpec((bm, HF), lambda n, i: (i + base, 0)), pl.BlockSpec((HF, B), lambda n, i: (0, n))]
                            + ([col, col] if own else []),
                            out_specs=[col])(ha, w2g, *([x, yr] if own else []), y if own else yp)

    barrier = pltpu.get_barrier_semaphore()
    friends = [peer, dev(nx, 0), dev(nx, 1), dev(ny, 0), dev(ny, 1)]
    for d in friends:
        pl.semaphore_signal(barrier, inc=1, device_id=(d,), device_id_type=MESH)
    pl.semaphore_wait(barrier, len(friends))

    for d in w1_out(0):
        d.start()
    cx.start()
    cg.start()
    pltpu.emit_pipeline(copy_body, grid=(4,), in_specs=[pl.BlockSpec((256, B), lambda i: (0, 2 * i + c))],
                        out_specs=[pl.BlockSpec((256, B), lambda i: (me, i))])(w1, w1g)
    for d in w1_in(0):
        d.wait_recv()
    for d in w1_relay(0):
        d.start()
    for d in w1_out(1):
        d.start()
    row = pl.BlockSpec((B, D), lambda i: (i, 0))
    pltpu.emit_pipeline(copy_body, grid=(TOK // B,), in_specs=[row, row], out_specs=[row, row])(
        x, g, xa.at[pl.ds(0, TOK)], ga.at[pl.ds(0, TOK)])
    pltpu.emit_pipeline(copy_body, grid=(2,), in_specs=[pl.BlockSpec((B // 2, D), lambda i: (i, 0))],
                        out_specs=[pl.BlockSpec((B // 2, D), lambda i: (2 * q + i, 0))])(w2, w2g)
    cx.wait_recv()

    @pl.loop(0, 4)
    def _(j):
        for d in w1_relay_in(j):
            d.wait_recv()
        a_phase(j)

    cg.wait_recv()
    d2(0, lambda i: nd, lambda i: i)
    p2[0].start()
    p2[1].start()
    for d in w2_in:
        d.wait_recv()
    for d in w2_relay:
        d.start()
    d2(2, near, lambda i: i)
    p2[2].start()
    p2[3].start()
    e_phase(0, 3)
    for d in w2_relay_in:
        d.wait_recv()
    e_phase(3, 1)
    d1(0, lambda i: nd, lambda i: i)
    p1d[0].start()
    p1d[1].start()
    p2[0].wait_recv()
    p2[1].wait_recv()
    d2(4, near, lambda i: 1 - i, [(r2, lambda i: 1 - i)])
    p2[4].start()
    p2[5].start()
    d1(2, near, lambda i: i)
    for k in (0, 1):
        for d in p1[k]:
            d.start()
    y_phase(False)
    cy.start()
    p1d[0].wait_recv()
    p1d[1].wait_recv()
    d1(4, near, lambda i: 1 - i, [(r1, lambda i: 1 - i)])
    for k in (2, 3):
        for d in p1[k]:
            d.start()
    tn(xa, da, o1, 512, D, lambda i: q, lambda i: i, half1)
    co.start()
    for k in range(2, 6):
        p2[k].wait_recv()
    tn(ha, ga, dw2, B, B, lambda i: q, lambda i: i, pl.BlockSpec((B, B), lambda i, k: (0, i)),
       [(r2, lambda i: 2 + i), (r2, lambda i: 5 - i)])
    cy.wait_recv()
    y_phase(True)
    co.wait_recv()
    for pair in p1_in:
        for d in pair:
            d.wait_recv()
    for d in [cx, cg, co, cy] + w2_out + w2_relay + p2 + p1d + [d for pair in p1 for d in pair]:
        d.wait_send()

    @pl.loop(0, 4)
    def _(j):
        for d in w1_out(j) + w1_relay(j):
            d.wait_send()


def solution(mesh):
    spec = P(None, AX, None)

    def body(x, g, w1, w2):
        c = lax.axis_index(AX) % 2
        shape = lambda s, t: jax.ShapeDtypeStruct(s, t)
        dma = lambda *s: pltpu.SemaphoreType.DMA(s)
        hbm = pl.BlockSpec(memory_space=pl.ANY)
        outs = [
            shape((TOK, D), BF16), shape((B, D), F32), shape((2, 512, D), F32), shape((2, 256, D), F32), shape((4, 2, 256, D), F32),
            shape((T, D), BF16), shape((T, D), BF16), shape((D, HF), BF16), shape((HF, D), BF16),
            shape((T, HF), BF16), shape((T, HF), BF16), shape((T, HF), BF16),
            shape((6, B, B), F32), shape((6, B, B), F32), shape((6, 512, D), F32), shape((2, 512, D), F32),
            shape((TOK, D), F32), shape((TOK, D), F32),
        ]
        res = pl.pallas_call(
            _kernel,
            out_shape=outs,
            in_specs=[hbm] * 4,
            out_specs=[hbm] * len(outs),
            scratch_shapes=[dma(2), dma(2), dma(4, 7), dma(4, 7), dma(4), dma(4), dma(6), dma(6), dma(6, 2), dma(6, 2),
                            dma(1), dma(1), dma(1), dma(1)],
            compiler_params=pltpu.CompilerParams(collective_id=0, has_side_effects=True, vmem_limit_bytes=VMEM),
            name="step",
        )(x.reshape(TOK, D), g.reshape(TOK, D), w1[0], w2[0])
        y, dw2, o1, o1r, r1f = res[:5]
        mine = lax.dynamic_slice_in_dim(o1, 256 * c, 256, 1)
        own = jnp.where(c == 0, jnp.stack([mine, o1r]), jnp.stack([o1r, mine]))
        far = jnp.stack([r1f[0] + r1f[3], r1f[1] + r1f[2]], axis=1)
        dw1 = (own + far).reshape(2, 2, 256, 2, B).transpose(2, 1, 3, 0, 4).reshape(1, 256, 8192)
        return y.reshape(2, TOK // 2, D), dw1, dw2[None]

    return jax.shard_map(body, mesh=mesh, in_specs=(spec, spec, spec, spec),
                         out_specs=(spec, spec, spec), check_vma=False)
```

```python
import functools

import jax
import jax.numpy as jnp
from jax import lax
from jax.experimental import pallas as pl
from jax.experimental.pallas import tpu as pltpu
from jax.sharding import PartitionSpec as P

AX = "fsdp"
F32 = jnp.float32
BF16 = jnp.bfloat16
MESH = pl.DeviceIdType.MESH
C0 = 0.7978845608028654
C1 = 0.044715
D = 2048
HF = 4096
TOK = 4096
T = 2 * TOK
B = 1024
SUB = 256
VMEM = 60 * 2**20


def _gelu(a):
    t = jnp.tanh(a * (C0 + (C0 * C1) * (a * a)))
    b = 0.5 * a
    return b + b * t


def _gelu_grad(a):
    a2 = a * a
    t = jnp.tanh(a * (C0 + (C0 * C1) * a2))
    return (0.5 + 0.5 * t) + ((1.0 - t * t) * a) * (0.5 * C0 + (1.5 * C0 * C1) * a2)


def _kernel(x, g, w1, w2,
            y, dw2, o1, o1r, r1f, xa, ga, w1g, w2g, aa, ha, da, s2, r2, s1, r1, yp, yr,
            xs, xr, w1s, w1r, w2s, w2r, s2s, s2r, s1s, s1r, os, orr, ys, yrs):
    me = lax.axis_index(AX)
    c, q = me % 2, me // 2
    qx, qy = q % 2, q // 2
    nx, ny, nd = 2 * qy + (1 - qx), 2 * (1 - qy) + qx, 3 - q
    dev = lambda chip, core: 2 * chip + core
    peer = dev(q, 1 - c)

    def blk(i):
        return 2 * ((qy + i // 2) % 2) + (qx + i % 2) % 2

    def rdma(src, dst, ss, rs, to):
        return pltpu.make_async_remote_copy(src_ref=src, dst_ref=dst, send_sem=ss, recv_sem=rs,
                                            device_id=(to,), device_id_type=MESH)

    cx = rdma(x, xa.at[pl.ds(TOK, TOK)], xs.at[0], xr.at[0], peer)
    cg = rdma(g, ga.at[pl.ds(TOK, TOK)], xs.at[1], xr.at[1], peer)

    def w1_rows(owner, j):
        return w1g.at[pl.ds(owner * 256, 256), pl.ds(j * B, B)]

    def w1_out(j):
        def one(role, rsem, p, to):
            return rdma(w1.at[:, pl.ds((2 * j + p) * B, B)], w1_rows(me, j), w1s.at[j, role], w1r.at[j, rsem], to)
        return [one(1, 1 + c, 0, dev(nx, 0)), one(2, 1 + c, 1, dev(nx, 1)),
                one(3, 3 + c, 0, dev(ny, 0)), one(4, 3 + c, 1, dev(ny, 1)),
                one(0, 0, 1 - c, peer)]

    def w1_in(j):
        def one(owner, rsem):
            return rdma(w1_rows(owner, j), w1_rows(owner, j), w1s.at[j, 0], w1r.at[j, rsem], peer)
        return [one(peer, 0), one(dev(nx, 0), 1), one(dev(nx, 1), 2), one(dev(ny, 0), 3), one(dev(ny, 1), 4)]

    def w1_relay(j):
        ra, rb = w1_rows(dev(nx, 0), j), w1_rows(dev(ny, 1), j)
        return [rdma(ra, ra, w1s.at[j, 5], w1r.at[j, 5], dev(ny, c)),
                rdma(rb, rb, w1s.at[j, 6], w1r.at[j, 6], dev(nx, c))]

    def w1_relay_in(j):
        ra, rb = w1_rows(dev(nd, 0), j), w1_rows(dev(nd, 1), j)
        return [rdma(ra, ra, w1s.at[j, 5], w1r.at[j, 5], peer), rdma(rb, rb, w1s.at[j, 6], w1r.at[j, 6], peer)]

    def w2_rows(chip, lo, n):
        return w2g.at[pl.ds(chip * B + lo, n)]

    w2_out = [rdma(w2, w2_rows(q, 0, B), w2s.at[0], w2r.at[0], dev(nx, c)),
              rdma(w2, w2_rows(q, 0, B), w2s.at[1], w2r.at[1], dev(ny, c))]
    w2_in = [rdma(w2_rows(nx, 0, B), w2_rows(nx, 0, B), w2s.at[0], w2r.at[0], peer),
             rdma(w2_rows(ny, 0, B), w2_rows(ny, 0, B), w2s.at[1], w2r.at[1], peer)]
    w2_relay = [rdma(w2_rows(nx, 0, B // 2), w2_rows(nx, 0, B // 2), w2s.at[2], w2r.at[2], dev(ny, c)),
                rdma(w2_rows(ny, B // 2, B // 2), w2_rows(ny, B // 2, B // 2), w2s.at[3], w2r.at[3], dev(nx, c))]
    w2_relay_in = [rdma(w2_rows(nd, 0, B // 2), w2_rows(nd, 0, B // 2), w2s.at[2], w2r.at[2], peer),
                   rdma(w2_rows(nd, B // 2, B // 2), w2_rows(nd, B // 2, B // 2), w2s.at[3], w2r.at[3], peer)]

    p2 = [rdma(s2.at[k], r2.at[k], s2s.at[k], s2r.at[k], dev(nx if k in (0, 2, 4) else ny, c)) for k in range(6)]
    p1d = [rdma(s1.at[k], r1.at[k], s1s.at[k, 0], s1r.at[k, 0], dev(nx if k == 0 else ny, c)) for k in range(2)]
    p1 = [[rdma(s1.at[k, pl.ds(256 * p, 256)], r1f.at[k - 2, c], s1s.at[k, p], s1r.at[k, c], dev(nx if k in (2, 4) else ny, p))
           for p in range(2)] for k in range(2, 6)]
    p1_in = [[rdma(s1.at[k, pl.ds(256 * p, 256)], r1f.at[k - 2, p], s1s.at[k, p], s1r.at[k, p], peer)
              for p in range(2)] for k in range(2, 6)]
    co = rdma(o1.at[:, pl.ds(256 * (1 - c), 256)], o1r, os.at[0], orr.at[0], peer)
    cy = rdma(yp, yr, ys.at[0], yrs.at[0], peer)

    def copy_body(*refs):
        n = len(refs) // 2
        for i in range(n):
            refs[n + i][...] = refs[i][...]

    def a_phase(j):
        def body(x_ref, w_ref, a_ref, h_ref):
            @pl.when((pl.program_id(0) == 6) & (j < 3))
            def _():
                for d in w1_in(j + 1):
                    d.wait_recv()
                for d in w1_relay(j + 1):
                    d.start()

            @pl.when((pl.program_id(0) == 6) & (j < 2))
            def _():
                for d in w1_out(j + 2):
                    d.start()

            @pl.when((pl.program_id(0) == 6) & (j == 2))
            def _():
                for d in w2_out:
                    d.start()

            for n in range(B // SUB):
                s = slice(n * SUB, (n + 1) * SUB)
                a = jnp.dot(x_ref[s, :], w_ref[...], preferred_element_type=F32).astype(BF16)
                a_ref[s, :] = a
                h_ref[s, :] = _gelu(a.astype(F32)).astype(BF16)

        out = pl.BlockSpec((B, B), lambda i: (i, j))
        pltpu.emit_pipeline(body, grid=(T // B,),
                            in_specs=[pl.BlockSpec((B, D), lambda i: (i, 0)), pl.BlockSpec((D, B), lambda i: (0, j))],
                            out_specs=[out, out])(xa, w1g, aa, ha)

    def e_phase(lo, n):
        def body(g_ref, w_ref, a_ref, d_ref):
            for m in range(B // SUB):
                s = slice(m * SUB, (m + 1) * SUB)
                e = lax.dot_general(g_ref[s, :], w_ref[...], (((1,), (1,)), ((), ())), preferred_element_type=F32)
                d_ref[s, :] = (_gelu_grad(a_ref[s, :].astype(F32)) * e).astype(BF16)

        act = pl.BlockSpec((B, B), lambda i, k: (k, blk(i + lo)))
        pltpu.emit_pipeline(body, grid=(n, T // B),
                            in_specs=[pl.BlockSpec((B, D), lambda i, k: (k, 0)),
                                      pl.BlockSpec((B, D), lambda i, k: (blk(i + lo), 0)), act],
                            out_specs=[act])(ga, w2g, aa, da)

    def tn(lhs, rhs, out, m, n, li, ri, out_spec, recv=()):
        def body(l_ref, r_ref, *rest):
            o_ref = rest[-1]
            @pl.when(pl.program_id(1) == 0)
            def _():
                init = jnp.zeros(o_ref.shape, F32)
                for r in rest[:-1]:
                    init = init + r[...].reshape(o_ref.shape)
                o_ref[...] = init
            for i in range(m // SUB):
                s = slice(i * SUB, (i + 1) * SUB)
                o_ref[..., s, :] += lax.dot_general(l_ref[:, s], r_ref[...], (((0,), (0,)), ((), ())),
                                                    preferred_element_type=F32).reshape(o_ref.shape[:-2] + (SUB, n))

        pltpu.emit_pipeline(body, grid=(2, T // B),
                            in_specs=[pl.BlockSpec((B, m), lambda i, k: (k, li(i))), pl.BlockSpec((B, n), lambda i, k: (k, ri(i)))]
                            + [pl.BlockSpec((1, m, n), functools.partial(lambda f, i, k: (f(i), 0, 0), f)) for _, f in recv],
                            out_specs=[out_spec])(lhs, rhs, *[r for r, _ in recv], out)

    half = pl.BlockSpec((1, B, B), lambda i, k: (i, 0, 0))
    half1 = pl.BlockSpec((1, 512, D), lambda i, k: (i, 0, 0))
    near = lambda i: (1 - i) * nx + i * ny
    d2 = lambda slot, li, ri, recv=(): tn(ha, ga, s2.at[pl.ds(slot, 2)], B, B, li, ri, half, recv)
    d1 = lambda slot, li, ri, recv=(): tn(xa, da, s1.at[pl.ds(slot, 2)], 512, D, li, ri, half1, recv)

    def y_phase(own):
        def body(h_ref, w_ref, *rest):
            v = jnp.dot(h_ref[...], w_ref[...], preferred_element_type=F32)
            if own:
                x_ref, r_ref, o_ref = rest
                o_ref[...] = (x_ref[...].astype(F32) + (v + r_ref[...])).astype(BF16)
            else:
                rest[0][...] = v

        bm = 512
        base = 0 if own else TOK // bm
        col = pl.BlockSpec((bm, B), lambda n, i: (i, n))
        pltpu.emit_pipeline(body, grid=(2, TOK // bm),
                            in_specs=[pl.BlockSpec((bm, HF), lambda n, i: (i + base, 0)), pl.BlockSpec((HF, B), lambda n, i: (0, n))]
                            + ([col, col] if own else []),
                            out_specs=[col])(ha, w2g, *([x, yr] if own else []), y if own else yp)

    barrier = pltpu.get_barrier_semaphore()
    friends = [peer, dev(nx, 0), dev(nx, 1), dev(ny, 0), dev(ny, 1)]
    for d in friends:
        pl.semaphore_signal(barrier, inc=1, device_id=(d,), device_id_type=MESH)
    pl.semaphore_wait(barrier, len(friends))

    for d in w1_out(0):
        d.start()
    cx.start()
    cg.start()
    pltpu.emit_pipeline(copy_body, grid=(4,), in_specs=[pl.BlockSpec((256, B), lambda i: (0, 2 * i + c))],
                        out_specs=[pl.BlockSpec((256, B), lambda i: (me, i))])(w1, w1g)
    for d in w1_in(0):
        d.wait_recv()
    for d in w1_relay(0):
        d.start()
    for d in w1_out(1):
        d.start()
    row = pl.BlockSpec((B, D), lambda i: (i, 0))
    pltpu.emit_pipeline(copy_body, grid=(TOK // B,), in_specs=[row, row], out_specs=[row, row])(
        x, g, xa.at[pl.ds(0, TOK)], ga.at[pl.ds(0, TOK)])
    pltpu.emit_pipeline(copy_body, grid=(2,), in_specs=[pl.BlockSpec((B // 2, D), lambda i: (i, 0))],
                        out_specs=[pl.BlockSpec((B // 2, D), lambda i: (2 * q + i, 0))])(w2, w2g)
    cx.wait_recv()

    @pl.loop(0, 4)
    def _(j):
        for d in w1_relay_in(j):
            d.wait_recv()
        with jax.named_scope("pa"):
            a_phase(j)

    cg.wait_recv()
    with jax.named_scope("d2diag"):
        d2(0, lambda i: nd, lambda i: i)
    p2[0].start()
    p2[1].start()
    for d in w2_in:
        d.wait_recv()
    for d in w2_relay:
        d.start()
    with jax.named_scope("d2raw"):
        d2(2, near, lambda i: i)
    p2[2].start()
    p2[3].start()
    with jax.named_scope("e3"):
        e_phase(0, 3)
    for d in w2_relay_in:
        d.wait_recv()
    with jax.named_scope("e1"):
        e_phase(3, 1)
    with jax.named_scope("d1diag"):
        d1(0, lambda i: nd, lambda i: i)
    p1d[0].start()
    p1d[1].start()
    p2[0].wait_recv()
    p2[1].wait_recv()
    with jax.named_scope("d2add"):
        d2(4, near, lambda i: 1 - i, [(r2, lambda i: 1 - i)])
    p2[4].start()
    p2[5].start()
    with jax.named_scope("d1raw"):
        d1(2, near, lambda i: i)
    for k in (0, 1):
        for d in p1[k]:
            d.start()
    with jax.named_scope("ypeer"):
        y_phase(False)
    cy.start()
    p1d[0].wait_recv()
    p1d[1].wait_recv()
    with jax.named_scope("d1add"):
        d1(4, near, lambda i: 1 - i, [(r1, lambda i: 1 - i)])
    for k in (2, 3):
        for d in p1[k]:
            d.start()
    with jax.named_scope("d1own"):
        tn(xa, da, o1, 512, D, lambda i: q, lambda i: i, half1)
    co.start()
    for k in range(2, 6):
        p2[k].wait_recv()
    with jax.named_scope("d2own"):
        tn(ha, ga, dw2, B, B, lambda i: q, lambda i: i, pl.BlockSpec((B, B), lambda i, k: (0, i)),
           [(r2, lambda i: 2 + i), (r2, lambda i: 5 - i)])
    cy.wait_recv()
    with jax.named_scope("yown"):
        y_phase(True)
    co.wait_recv()
    for pair in p1_in:
        for d in pair:
            d.wait_recv()
    for d in [cx, cg, co, cy] + w2_out + w2_relay + p2 + p1d + [d for pair in p1 for d in pair]:
        d.wait_send()

    @pl.loop(0, 4)
    def _(j):
        for d in w1_out(j) + w1_relay(j):
            d.wait_send()


def _finish(c_ref, y, dw2, o1, o1r, fa, fb, y_out, dw1_out, dw2_out):
    y_out[...] = y[...]
    dw2_out[...] = dw2[...]
    own = jnp.where(pl.program_id(0) < 8, o1[0], o1r[0])
    dw1_out[...] = own + (fa[0, 0] + fb[0, 0])


def solution(mesh):
    spec = P(None, AX, None)

    def body(x, g, w1, w2):
        c = lax.axis_index(AX) % 2
        shape = lambda s, t: jax.ShapeDtypeStruct(s, t)
        dma = lambda *s: pltpu.SemaphoreType.DMA(s)
        hbm = pl.BlockSpec(memory_space=pl.ANY)
        outs = [
            shape((TOK, D), BF16), shape((B, D), F32), shape((2, 512, D), F32), shape((2, 256, D), F32), shape((4, 2, 256, D), F32),
            shape((T, D), BF16), shape((T, D), BF16), shape((D, HF), BF16), shape((HF, D), BF16),
            shape((T, HF), BF16), shape((T, HF), BF16), shape((T, HF), BF16),
            shape((6, B, B), F32), shape((6, B, B), F32), shape((6, 512, D), F32), shape((2, 512, D), F32),
            shape((TOK, D), F32), shape((TOK, D), F32),
        ]
        res = pl.pallas_call(
            _kernel,
            out_shape=outs,
            in_specs=[hbm] * 4,
            out_specs=[hbm] * len(outs),
            scratch_shapes=[dma(2), dma(2), dma(4, 7), dma(4, 7), dma(4), dma(4), dma(6), dma(6), dma(6, 2), dma(6, 2),
                            dma(1), dma(1), dma(1), dma(1)],
            compiler_params=pltpu.CompilerParams(collective_id=0, has_side_effects=True, vmem_limit_bytes=VMEM),
            name="step",
        )(x.reshape(TOK, D), g.reshape(TOK, D), w1[0], w2[0])
        y, dw2, o1, o1r, r1f = res[:5]
        part = lambda s, c: (s // 8) * (1 - c[0]) + (1 - s // 8) * c[0]
        n, t, r = (lambda s: (s // 4) % 2), (lambda s: (s // 2) % 2), (lambda s: s % 2)
        mine = lambda s: jnp.minimum(s, 7)
        other = lambda s: jnp.maximum(s, 8)
        y_spec = pl.BlockSpec((TOK // 16, D), lambda s, c: (s, 0))
        dw2_spec = pl.BlockSpec((B // 16, D), lambda s, c: (s, 0))
        y, dw1, dw2 = pl.pallas_call(
            _finish,
            grid_spec=pltpu.PrefetchScalarGridSpec(
                num_scalar_prefetch=1,
                grid=(16,),
                in_specs=[
                    y_spec, dw2_spec,
                    pl.BlockSpec((1, 128, B), lambda s, c: (n(mine(s)), 2 * c[0] + r(mine(s)), t(mine(s)))),
                    pl.BlockSpec((1, 128, B), lambda s, c: (n(other(s)), r(other(s)), t(other(s)))),
                    pl.BlockSpec((1, 1, 128, B), lambda s, c: (n(s), part(s, c), r(s), t(s))),
                    pl.BlockSpec((1, 1, 128, B), lambda s, c: (3 - n(s), part(s, c), r(s), t(s))),
                ],
                out_specs=[y_spec, pl.BlockSpec((128, B), lambda s, c: (r(s), 2 * (2 * n(s) + t(s)) + part(s, c))), dw2_spec],
            ),
            out_shape=[shape((TOK, D), BF16), shape((256, 8192), F32), shape((B, D), F32)],
            compiler_params=pltpu.CompilerParams(dimension_semantics=("arbitrary",)),
            name="finish",
        )(c[None], y, dw2, o1, o1r, r1f, r1f)
        return y.reshape(2, TOK // 2, D), dw1[None], dw2[None]

    return jax.shard_map(body, mesh=mesh, in_specs=(spec, spec, spec, spec),
                         out_specs=(spec, spec, spec), check_vma=False)
```

```python
import functools

import jax
import jax.numpy as jnp
from jax import lax
from jax.experimental import pallas as pl
from jax.experimental.pallas import tpu as pltpu
from jax.sharding import PartitionSpec as P

AX = "fsdp"
F32 = jnp.float32
BF16 = jnp.bfloat16
MESH = pl.DeviceIdType.MESH
C0 = 0.7978845608028654
C1 = 0.044715
D = 2048
HF = 4096
TOK = 4096
T = 2 * TOK
B = 1024
SUB = 256
VMEM = 60 * 2**20


def _gelu(a):
    t = jnp.tanh(a * (C0 + (C0 * C1) * (a * a)))
    b = 0.5 * a
    return b + b * t


def _gelu_grad(a):
    a2 = a * a
    t = jnp.tanh(a * (C0 + (C0 * C1) * a2))
    return (0.5 + 0.5 * t) + ((1.0 - t * t) * a) * (0.5 * C0 + (1.5 * C0 * C1) * a2)


def _kernel(x, g, w1, w2,
            ha, w2g, yr, y0, dw2, s1, o1r, r1f, xa, ga, w1g, aa, da, s2, r2, r1, yp,
            xs, xr, w1s, w1r, w2s, w2r, s2s, s2r, s1s, s1r, os, orr, ys, yrs):
    me = lax.axis_index(AX)
    c, q = me % 2, me // 2
    qx, qy = q % 2, q // 2
    nx, ny, nd = 2 * qy + (1 - qx), 2 * (1 - qy) + qx, 3 - q
    dev = lambda chip, core: 2 * chip + core
    peer = dev(q, 1 - c)

    def blk(i):
        return 2 * ((qy + i // 2) % 2) + (qx + i % 2) % 2

    def rdma(src, dst, ss, rs, to):
        return pltpu.make_async_remote_copy(src_ref=src, dst_ref=dst, send_sem=ss, recv_sem=rs,
                                            device_id=(to,), device_id_type=MESH)

    cx = rdma(x, xa.at[pl.ds(TOK, TOK)], xs.at[0], xr.at[0], peer)
    cg = rdma(g, ga.at[pl.ds(TOK, TOK)], xs.at[1], xr.at[1], peer)

    def w1_rows(owner, j):
        return w1g.at[pl.ds(owner * 256, 256), pl.ds(j * B, B)]

    def w1_out(j):
        def one(role, rsem, p, to):
            return rdma(w1.at[:, pl.ds((2 * j + p) * B, B)], w1_rows(me, j), w1s.at[j, role], w1r.at[j, rsem], to)
        return [one(1, 1 + c, 0, dev(nx, 0)), one(2, 1 + c, 1, dev(nx, 1)),
                one(3, 3 + c, 0, dev(ny, 0)), one(4, 3 + c, 1, dev(ny, 1)),
                one(0, 0, 1 - c, peer)]

    def w1_in(j):
        def one(owner, rsem):
            return rdma(w1_rows(owner, j), w1_rows(owner, j), w1s.at[j, 0], w1r.at[j, rsem], peer)
        return [one(peer, 0), one(dev(nx, 0), 1), one(dev(nx, 1), 2), one(dev(ny, 0), 3), one(dev(ny, 1), 4)]

    def w1_relay(j):
        ra, rb = w1_rows(dev(nx, 0), j), w1_rows(dev(ny, 1), j)
        return [rdma(ra, ra, w1s.at[j, 5], w1r.at[j, 5], dev(ny, c)),
                rdma(rb, rb, w1s.at[j, 6], w1r.at[j, 6], dev(nx, c))]

    def w1_relay_in(j):
        ra, rb = w1_rows(dev(nd, 0), j), w1_rows(dev(nd, 1), j)
        return [rdma(ra, ra, w1s.at[j, 5], w1r.at[j, 5], peer), rdma(rb, rb, w1s.at[j, 6], w1r.at[j, 6], peer)]

    def w2_rows(chip, lo, n):
        return w2g.at[pl.ds(chip * B + lo, n)]

    w2_out = [rdma(w2, w2_rows(q, 0, B), w2s.at[0], w2r.at[0], dev(nx, c)),
              rdma(w2, w2_rows(q, 0, B), w2s.at[1], w2r.at[1], dev(ny, c))]
    w2_in = [rdma(w2_rows(nx, 0, B), w2_rows(nx, 0, B), w2s.at[0], w2r.at[0], peer),
             rdma(w2_rows(ny, 0, B), w2_rows(ny, 0, B), w2s.at[1], w2r.at[1], peer)]
    w2_relay = [rdma(w2_rows(nx, 0, B // 2), w2_rows(nx, 0, B // 2), w2s.at[2], w2r.at[2], dev(ny, c)),
                rdma(w2_rows(ny, B // 2, B // 2), w2_rows(ny, B // 2, B // 2), w2s.at[3], w2r.at[3], dev(nx, c))]
    w2_relay_in = [rdma(w2_rows(nd, 0, B // 2), w2_rows(nd, 0, B // 2), w2s.at[2], w2r.at[2], peer),
                   rdma(w2_rows(nd, B // 2, B // 2), w2_rows(nd, B // 2, B // 2), w2s.at[3], w2r.at[3], peer)]

    p2 = [rdma(s2.at[k], r2.at[k], s2s.at[k], s2r.at[k], dev(nx if k in (0, 2, 4) else ny, c)) for k in range(6)]
    p1d = [rdma(s1.at[k], r1.at[k], s1s.at[k, 0], s1r.at[k, 0], dev(nx if k == 0 else ny, c)) for k in range(2)]
    p1 = [[rdma(s1.at[k, pl.ds(256 * p, 256)], r1f.at[k - 2, c], s1s.at[k, p], s1r.at[k, c], dev(nx if k in (2, 4) else ny, p))
           for p in range(2)] for k in range(2, 6)]
    p1_in = [[rdma(s1.at[k, pl.ds(256 * p, 256)], r1f.at[k - 2, p], s1s.at[k, p], s1r.at[k, p], peer)
              for p in range(2)] for k in range(2, 6)]
    co = rdma(s1.at[pl.ds(6, 2), pl.ds(256 * (1 - c), 256)], o1r, os.at[0], orr.at[0], peer)
    cy = rdma(yp, yr, ys.at[0], yrs.at[0], peer)

    def copy_body(*refs):
        n = len(refs) // 2
        for i in range(n):
            refs[n + i][...] = refs[i][...]

    def a_phase():
        def body(x_ref, w_ref, a_ref, h_ref):
            j, k = pl.program_id(0), pl.program_id(1)

            @pl.when((k == 4) & (j < 3))
            def _():
                for d in w1_in(j + 1):
                    d.wait_recv()
                for d in w1_relay(j + 1):
                    d.start()

            @pl.when((k == 4) & (j < 2))
            def _():
                for d in w1_out(j + 2):
                    d.start()

            @pl.when((k == 4) & (j == 2))
            def _():
                for d in w2_out:
                    d.start()

            @pl.when((k == 6) & (j < 3))
            def _():
                for d in w1_relay_in(j + 1):
                    d.wait_recv()

            for n in range(B // SUB):
                s = slice(n * SUB, (n + 1) * SUB)
                a = jnp.dot(x_ref[s, :], w_ref[...], preferred_element_type=F32).astype(BF16)
                a_ref[s, :] = a
                h_ref[s, :] = _gelu(a.astype(F32)).astype(BF16)

        out = pl.BlockSpec((B, B), lambda j, k: (k, j))
        pltpu.emit_pipeline(body, grid=(4, T // B),
                            in_specs=[pl.BlockSpec((B, D), lambda j, k: (k, 0)), pl.BlockSpec((D, B), lambda j, k: (0, j))],
                            out_specs=[out, out])(xa, w1g, aa, ha)

    def e_phase(lo, n):
        def body(g_ref, w_ref, a_ref, d_ref):
            for m in range(B // SUB):
                s = slice(m * SUB, (m + 1) * SUB)
                e = lax.dot_general(g_ref[s, :], w_ref[...], (((1,), (1,)), ((), ())), preferred_element_type=F32)
                d_ref[s, :] = (_gelu_grad(a_ref[s, :].astype(F32)) * e).astype(BF16)

        act = pl.BlockSpec((B, B), lambda i, k: (k, blk(i + lo)))
        pltpu.emit_pipeline(body, grid=(n, T // B),
                            in_specs=[pl.BlockSpec((B, D), lambda i, k: (k, 0)),
                                      pl.BlockSpec((B, D), lambda i, k: (blk(i + lo), 0)), act],
                            out_specs=[act])(ga, w2g, aa, da)

    MS = 512

    def tn(parts, lhs, rhs, out, m, n, li, ri, out_spec, recv=(), at=None):
        def body(l_ref, r_ref, *rest):
            o_ref = rest[-1]
            if at is not None:
                @pl.when(pl.program_id(1) == 1)
                def _():
                    at(pl.program_id(0))

            @pl.when(pl.program_id(1) == 0)
            def _():
                o_ref[...] = jnp.zeros(o_ref.shape, F32)

            for r in rest[:-1]:
                @pl.when((pl.program_id(1) == 0) & (pl.program_id(0) < 2))
                def _():
                    o_ref[...] += r[...].reshape(o_ref.shape)

            for i in range(m // MS):
                s = slice(i * MS, (i + 1) * MS)
                o_ref[..., s, :] += lax.dot_general(l_ref[:, s], r_ref[...], (((0,), (0,)), ((), ())),
                                                    preferred_element_type=F32).reshape(o_ref.shape[:-2] + (MS, n))

        kt = 2048 if parts == 4 else B
        pltpu.emit_pipeline(body, grid=(parts, T // kt),
                            in_specs=[pl.BlockSpec((kt, m), lambda i, k: (k, li(i))), pl.BlockSpec((kt, n), lambda i, k: (k, ri(i)))]
                            + [pl.BlockSpec((1, m, n), functools.partial(lambda f, i, k: (f(i), 0, 0), f)) for _, f in recv],
                            out_specs=[out_spec])(lhs, rhs, *[r for r, _ in recv], out)

    half = pl.BlockSpec((1, B, B), lambda i, k: (i, 0, 0))
    half1 = pl.BlockSpec((1, 512, D), lambda i, k: (i, 0, 0))

    def first(i):
        return jnp.where(i < 2, nd, jnp.where(i == 2, nx, ny))

    def last(i):
        return jnp.where(i == 0, nx, jnp.where(i == 1, ny, q))

    other = lambda i: jnp.where(i == 0, 1, jnp.where(i == 1, 0, i - 2))

    def y_phase(own):
        def body(h_ref, w_ref, *rest):
            v = jnp.dot(h_ref[...], w_ref[...], preferred_element_type=F32)
            if own:
                x_ref, r_ref, o_ref = rest
                o_ref[...] = (x_ref[...].astype(F32) + (v + r_ref[...])).astype(BF16)
            else:
                rest[0][...] = v

        bm = 512
        base = 0 if own else TOK // bm
        col = pl.BlockSpec((bm, B), lambda n, i: (i, n))
        pltpu.emit_pipeline(body, grid=(2, (TOK // 2 if own else TOK) // bm),
                            in_specs=[pl.BlockSpec((bm, HF), lambda n, i: (i + base, 0)), pl.BlockSpec((HF, B), lambda n, i: (0, n))]
                            + ([col, col] if own else []),
                            out_specs=[col])(ha, w2g, *([x, yr] if own else []), y0 if own else yp)

    barrier = pltpu.get_barrier_semaphore()
    friends = [peer, dev(nx, 0), dev(nx, 1), dev(ny, 0), dev(ny, 1)]
    for d in friends:
        pl.semaphore_signal(barrier, inc=1, device_id=(d,), device_id_type=MESH)
    pl.semaphore_wait(barrier, len(friends))

    for d in w1_out(0):
        d.start()
    cx.start()
    cg.start()
    row = pl.BlockSpec((B, D), lambda i: (i, 0))
    pltpu.emit_pipeline(copy_body, grid=(4,),
                        in_specs=[pl.BlockSpec((256, B), lambda i: (0, 2 * i + c)), row],
                        out_specs=[pl.BlockSpec((256, B), lambda i: (me, i)), row])(w1, x, w1g, xa.at[pl.ds(0, TOK)])
    for d in w1_in(0):
        d.wait_recv()
    for d in w1_relay(0):
        d.start()
    for d in w1_out(1):
        d.start()
    pltpu.emit_pipeline(copy_body, grid=(4,),
                        in_specs=[pl.BlockSpec((256, D), lambda i: (i, 0)), row],
                        out_specs=[pl.BlockSpec((256, D), lambda i: (4 * q + i, 0)), row])(w2, g, w2g, ga.at[pl.ds(0, TOK)])
    cx.wait_recv()
    for d in w1_relay_in(0):
        d.wait_recv()
    with jax.named_scope("pa"):
        a_phase()
    cg.wait_recv()

    def at2(i):
        @pl.when(i == 1)
        def _():
            p2[0].start()

        @pl.when(i == 2)
        def _():
            p2[1].start()
            for d in w2_in:
                d.wait_recv()
            for d in w2_relay:
                d.start()

        @pl.when(i == 3)
        def _():
            p2[2].start()

    with jax.named_scope("d2diag"):
        tn(4, ha, ga, s2.at[pl.ds(0, 4)], B, B, first, lambda i: i % 2, half, at=at2)
    p2[3].start()
    with jax.named_scope("e3"):
        e_phase(0, 3)
    p2[0].wait_recv()
    p2[1].wait_recv()
    with jax.named_scope("d2add"):
        tn(2, ha, ga, s2.at[pl.ds(4, 2)], B, B, last, other, half, [(r2, lambda i: 1 - i)])
    p2[4].start()
    p2[5].start()
    for d in w2_relay_in:
        d.wait_recv()
    with jax.named_scope("e1"):
        e_phase(3, 1)

    def at1(i):
        @pl.when(i == 1)
        def _():
            p1d[0].start()

        @pl.when(i == 2)
        def _():
            p1d[1].start()

        @pl.when(i == 3)
        def _():
            for d in p1[0]:
                d.start()

    with jax.named_scope("d1diag"):
        tn(4, xa, da, s1.at[pl.ds(0, 4)], 512, D, first, lambda i: i % 2, half1, at=at1)
    for d in p1[1]:
        d.start()
    with jax.named_scope("ypeer"):
        y_phase(False)
    cy.start()
    p1d[0].wait_recv()
    p1d[1].wait_recv()

    def at1s(i):
        for k in (2, 3):
            @pl.when(i == k - 1)
            def _():
                for d in p1[k]:
                    d.start()

    with jax.named_scope("d1add"):
        tn(4, xa, da, s1.at[pl.ds(4, 4)], 512, D, last, other, half1, [(r1, lambda i: jnp.where(i == 0, 1, 0))], at=at1s)
    co.start()
    for k in range(2, 6):
        p2[k].wait_recv()
    with jax.named_scope("d2own"):
        tn(2, ha, ga, dw2, B, B, lambda i: q, lambda i: i, pl.BlockSpec((B, B), lambda i, k: (0, i)),
           [(r2, lambda i: 2 + i), (r2, lambda i: 5 - i)])
    cy.wait_recv()
    with jax.named_scope("yown"):
        y_phase(True)
    co.wait_recv()
    for pair in p1_in:
        for d in pair:
            d.wait_recv()
    for d in [cx, cg, co, cy] + w2_out + w2_relay + p2 + p1d + [d for pair in p1 for d in pair]:
        d.wait_send()

    @pl.loop(0, 4)
    def _(j):
        for d in w1_out(j) + w1_relay(j):
            d.wait_send()


def _finish(c_ref, h, w2, x, yr, y0, dw2, o1, o1r, fa, fb, y_out, dw1_out, dw2_out):
    for n in range(2):
        s = slice(n * B, (n + 1) * B)
        v = jnp.dot(h[...], w2[:, s], preferred_element_type=F32)
        y_out[1, :, s] = (x[:, s].astype(F32) + (v + yr[:, s])).astype(BF16)
    y_out[0] = y0[...]
    dw2_out[...] = dw2[...]
    own = jnp.where(pl.program_id(0) < 4, o1[0], o1r[0])
    dw1_out[...] = own + (fa[0, 0] + fb[0, 0])


def solution(mesh):
    spec = P(None, AX, None)

    def body(x, g, w1, w2):
        c = lax.axis_index(AX) % 2
        shape = lambda s, t: jax.ShapeDtypeStruct(s, t)
        dma = lambda *s: pltpu.SemaphoreType.DMA(s)
        hbm = pl.BlockSpec(memory_space=pl.ANY)
        x = x.reshape(TOK, D)
        outs = [
            shape((T, HF), BF16), shape((HF, D), BF16), shape((TOK, D), F32), shape((TOK // 2, D), BF16), shape((B, D), F32),
            shape((8, 512, D), F32), shape((2, 256, D), F32), shape((4, 2, 256, D), F32),
            shape((T, D), BF16), shape((T, D), BF16), shape((D, HF), BF16), shape((T, HF), BF16), shape((T, HF), BF16),
            shape((6, B, B), F32), shape((6, B, B), F32), shape((2, 512, D), F32), shape((TOK, D), F32),
        ]
        res = pl.pallas_call(
            _kernel,
            out_shape=outs,
            in_specs=[hbm] * 4,
            out_specs=[hbm] * len(outs),
            scratch_shapes=[dma(2), dma(2), dma(4, 7), dma(4, 7), dma(4), dma(4), dma(6), dma(6), dma(6, 2), dma(6, 2),
                            dma(1), dma(1), dma(1), dma(1)],
            compiler_params=pltpu.CompilerParams(collective_id=0, has_side_effects=True, vmem_limit_bytes=VMEM),
            name="step",
        )(x, g.reshape(TOK, D), w1[0], w2[0])
        h, w2g, yr, y0, dw2, s1, o1r, r1f = res[:8]
        part = lambda s, c: (s // 4) * (1 - c[0]) + (1 - s // 4) * c[0]
        n, t = (lambda s: (s // 2) % 2), (lambda s: s % 2)
        mine = lambda s: jnp.minimum(s, 3)
        theirs = lambda s: jnp.maximum(s, 4)
        bm = TOK // 16
        row = lambda m, w=D, lo=0: pl.BlockSpec((m, w), lambda s, c: (s + lo, 0))
        y, dw1, dw2 = pl.pallas_call(
            _finish,
            grid_spec=pltpu.PrefetchScalarGridSpec(
                num_scalar_prefetch=1,
                grid=(8,),
                in_specs=[
                    row(bm, HF, 8), pl.BlockSpec((HF, D), lambda s, c: (0, 0), pipeline_mode=pl.Buffered(1)), row(bm, D, 8), row(bm, D, 8),
                    row(bm), row(B // 8),
                    pl.BlockSpec((1, 256, B), lambda s, c: (6 + n(mine(s)), c[0], t(mine(s)))),
                    pl.BlockSpec((1, 256, B), lambda s, c: (n(theirs(s)), 0, t(theirs(s)))),
                    pl.BlockSpec((1, 1, 256, B), lambda s, c: (n(s), part(s, c), 0, t(s))),
                    pl.BlockSpec((1, 1, 256, B), lambda s, c: (3 - n(s), part(s, c), 0, t(s))),
                ],
                out_specs=[pl.BlockSpec((2, bm, D), lambda s, c: (0, s, 0)), pl.BlockSpec((256, B), lambda s, c: (0, 2 * (2 * n(s) + t(s)) + part(s, c))), row(B // 8)],
            ),
            out_shape=[shape((2, TOK // 2, D), BF16), shape((256, 8192), F32), shape((B, D), F32)],
            compiler_params=pltpu.CompilerParams(dimension_semantics=("arbitrary",), vmem_limit_bytes=VMEM),
            name="finish",
        )(c[None], h, w2g, x, yr, y0, dw2, s1, o1r, r1f, r1f)
        return y, dw1[None], dw2[None]

    return jax.shard_map(body, mesh=mesh, in_specs=(spec, spec, spec, spec),
                         out_specs=(spec, spec, spec), check_vma=False)
```

```python
import functools

import jax
import jax.numpy as jnp
from jax import lax
from jax.experimental import pallas as pl
from jax.experimental.pallas import tpu as pltpu
from jax.sharding import PartitionSpec as P

AX = "fsdp"
F32 = jnp.float32
BF16 = jnp.bfloat16
MESH = pl.DeviceIdType.MESH
C0 = 0.7978845608028654
C1 = 0.044715
D = 2048
HF = 4096
TOK = 4096
T = 2 * TOK
B = 1024
SUB = 256
VMEM = 60 * 2**20


def _gelu(a):
    t = jnp.tanh(a * (C0 + (C0 * C1) * (a * a)))
    b = 0.5 * a
    return b + b * t


def _gelu_grad(a):
    a2 = a * a
    t = jnp.tanh(a * (C0 + (C0 * C1) * a2))
    return (0.5 + 0.5 * t) + ((1.0 - t * t) * a) * (0.5 * C0 + (1.5 * C0 * C1) * a2)


def _kernel(x, g, w1, w2,
            ha, w2g, yr, y0, dw2, s1, o1r, r1f, xa, ga, w1g, aa, da, s2, r2, r1, yp,
            xs, xr, w1s, w1r, w2s, w2r, s2s, s2r, s1s, s1r, os, orr, ys, yrs):
    me = lax.axis_index(AX)
    c, q = me % 2, me // 2
    qx, qy = q % 2, q // 2
    nx, ny, nd = 2 * qy + (1 - qx), 2 * (1 - qy) + qx, 3 - q
    dev = lambda chip, core: 2 * chip + core
    peer = dev(q, 1 - c)

    def blk(i):
        return 2 * ((qy + i // 2) % 2) + (qx + i % 2) % 2

    def rdma(src, dst, ss, rs, to):
        return pltpu.make_async_remote_copy(src_ref=src, dst_ref=dst, send_sem=ss, recv_sem=rs,
                                            device_id=(to,), device_id_type=MESH)

    cx = rdma(x, xa.at[pl.ds(TOK, TOK)], xs.at[0], xr.at[0], peer)
    cg = rdma(g, ga.at[pl.ds(TOK, TOK)], xs.at[1], xr.at[1], peer)

    def w1_rows(owner, j):
        return w1g.at[pl.ds(owner * 256, 256), pl.ds(j * B, B)]

    def w1_out(j):
        def one(role, rsem, p, to):
            return rdma(w1.at[:, pl.ds((2 * j + p) * B, B)], w1_rows(me, j), w1s.at[j, role], w1r.at[j, rsem], to)
        return [one(1, 1 + c, 0, dev(nx, 0)), one(2, 1 + c, 1, dev(nx, 1)),
                one(3, 3 + c, 0, dev(ny, 0)), one(4, 3 + c, 1, dev(ny, 1)),
                one(0, 0, 1 - c, peer)]

    def w1_in(j):
        def one(owner, rsem):
            return rdma(w1_rows(owner, j), w1_rows(owner, j), w1s.at[j, 0], w1r.at[j, rsem], peer)
        return [one(peer, 0), one(dev(nx, 0), 1), one(dev(nx, 1), 2), one(dev(ny, 0), 3), one(dev(ny, 1), 4)]

    def w1_relay(j):
        ra, rb = w1_rows(dev(nx, 0), j), w1_rows(dev(ny, 1), j)
        return [rdma(ra, ra, w1s.at[j, 5], w1r.at[j, 5], dev(ny, c)),
                rdma(rb, rb, w1s.at[j, 6], w1r.at[j, 6], dev(nx, c))]

    def w1_relay_in(j):
        ra, rb = w1_rows(dev(nd, 0), j), w1_rows(dev(nd, 1), j)
        return [rdma(ra, ra, w1s.at[j, 5], w1r.at[j, 5], peer), rdma(rb, rb, w1s.at[j, 6], w1r.at[j, 6], peer)]

    def w2_rows(chip, lo, n):
        return w2g.at[pl.ds(chip * B + lo, n)]

    w2_out = [rdma(w2, w2_rows(q, 0, B), w2s.at[0], w2r.at[0], dev(nx, c)),
              rdma(w2, w2_rows(q, 0, B), w2s.at[1], w2r.at[1], dev(ny, c))]
    w2_in = [rdma(w2_rows(nx, 0, B), w2_rows(nx, 0, B), w2s.at[0], w2r.at[0], peer),
             rdma(w2_rows(ny, 0, B), w2_rows(ny, 0, B), w2s.at[1], w2r.at[1], peer)]
    w2_relay = [rdma(w2_rows(nx, 0, B // 2), w2_rows(nx, 0, B // 2), w2s.at[2], w2r.at[2], dev(ny, c)),
                rdma(w2_rows(ny, B // 2, B // 2), w2_rows(ny, B // 2, B // 2), w2s.at[3], w2r.at[3], dev(nx, c))]
    w2_relay_in = [rdma(w2_rows(nd, 0, B // 2), w2_rows(nd, 0, B // 2), w2s.at[2], w2r.at[2], peer),
                   rdma(w2_rows(nd, B // 2, B // 2), w2_rows(nd, B // 2, B // 2), w2s.at[3], w2r.at[3], peer)]

    p2 = [rdma(s2.at[k], r2.at[k], s2s.at[k], s2r.at[k], dev(nx if k in (0, 2, 4) else ny, c)) for k in range(6)]
    p1d = [rdma(s1.at[k], r1.at[k], s1s.at[k, 0], s1r.at[k, 0], dev(nx if k == 0 else ny, c)) for k in range(2)]
    p1 = [[rdma(s1.at[k, pl.ds(256 * p, 256)], r1f.at[k - 2, c], s1s.at[k, p], s1r.at[k, c], dev(nx if k in (2, 4) else ny, p))
           for p in range(2)] for k in range(2, 6)]
    p1_in = [[rdma(s1.at[k, pl.ds(256 * p, 256)], r1f.at[k - 2, p], s1s.at[k, p], s1r.at[k, p], peer)
              for p in range(2)] for k in range(2, 6)]
    co = rdma(s1.at[pl.ds(6, 2), pl.ds(256 * (1 - c), 256)], o1r, os.at[0], orr.at[0], peer)
    cy = rdma(yp, yr, ys.at[0], yrs.at[0], peer)

    def copy_body(*refs):
        n = len(refs) // 2
        for i in range(n):
            refs[n + i][...] = refs[i][...]

    def a_phase():
        def body(x_ref, w_ref, a_ref, h_ref):
            j, k = pl.program_id(0), pl.program_id(1)

            @pl.when((k == 4) & (j < 3))
            def _():
                for d in w1_in(j + 1):
                    d.wait_recv()
                for d in w1_relay(j + 1):
                    d.start()

            @pl.when((k == 4) & (j < 2))
            def _():
                for d in w1_out(j + 2):
                    d.start()

            @pl.when((k == 4) & (j == 2))
            def _():
                for d in w2_out:
                    d.start()

            @pl.when((k == 6) & (j < 3))
            def _():
                for d in w1_relay_in(j + 1):
                    d.wait_recv()

            for n in range(B // SUB):
                s = slice(n * SUB, (n + 1) * SUB)
                a = jnp.dot(x_ref[s, :], w_ref[...], preferred_element_type=F32).astype(BF16)
                a_ref[s, :] = a
                h_ref[s, :] = _gelu(a.astype(F32)).astype(BF16)

        out = pl.BlockSpec((B, B), lambda j, k: (k, j))
        pltpu.emit_pipeline(body, grid=(4, T // B),
                            in_specs=[pl.BlockSpec((B, D), lambda j, k: (k, 0)), pl.BlockSpec((D, B), lambda j, k: (0, j))],
                            out_specs=[out, out])(xa, w1g, aa, ha)

    def e_phase(lo, n):
        def body(g_ref, w_ref, a_ref, d_ref):
            for m in range(B // SUB):
                s = slice(m * SUB, (m + 1) * SUB)
                e = lax.dot_general(g_ref[s, :], w_ref[...], (((1,), (1,)), ((), ())), preferred_element_type=F32)
                d_ref[s, :] = (_gelu_grad(a_ref[s, :].astype(F32)) * e).astype(BF16)

        act = pl.BlockSpec((B, B), lambda i, k: (k, blk(i + lo)))
        pltpu.emit_pipeline(body, grid=(n, T // B),
                            in_specs=[pl.BlockSpec((B, D), lambda i, k: (k, 0)),
                                      pl.BlockSpec((B, D), lambda i, k: (blk(i + lo), 0)), act],
                            out_specs=[act])(ga, w2g, aa, da)

    MS = 512

    def tn(parts, lhs, rhs, out, m, n, li, ri, out_spec, recv=(), at=None):
        def body(l_ref, r_ref, *rest):
            o_ref = rest[-1]
            if at is not None:
                @pl.when(pl.program_id(1) == 1)
                def _():
                    at(pl.program_id(0))

            @pl.when(pl.program_id(1) == 0)
            def _():
                o_ref[...] = jnp.zeros(o_ref.shape, F32)

            for r in rest[:-1]:
                @pl.when((pl.program_id(1) == 0) & (pl.program_id(0) < 2))
                def _():
                    o_ref[...] += r[...].reshape(o_ref.shape)

            for i in range(m // MS):
                s = slice(i * MS, (i + 1) * MS)
                o_ref[..., s, :] += lax.dot_general(l_ref[:, s], r_ref[...], (((0,), (0,)), ((), ())),
                                                    preferred_element_type=F32).reshape(o_ref.shape[:-2] + (MS, n))

        kt = B
        pltpu.emit_pipeline(body, grid=(parts, T // kt),
                            in_specs=[pl.BlockSpec((kt, m), lambda i, k: (k, li(i))), pl.BlockSpec((kt, n), lambda i, k: (k, ri(i)))]
                            + [pl.BlockSpec((1, m, n), functools.partial(lambda f, i, k: (f(i), 0, 0), f)) for _, f in recv],
                            out_specs=[out_spec])(lhs, rhs, *[r for r, _ in recv], out)

    half = pl.BlockSpec((1, B, B), lambda i, k: (i, 0, 0))
    half1 = pl.BlockSpec((1, 512, D), lambda i, k: (i, 0, 0))

    def first(i):
        return jnp.where(i < 2, nd, jnp.where(i == 2, nx, ny))

    def last(i):
        return jnp.where(i == 0, nx, jnp.where(i == 1, ny, q))

    other = lambda i: jnp.where(i == 0, 1, jnp.where(i == 1, 0, i - 2))

    def y_phase(own):
        def body(h_ref, w_ref, *rest):
            v = jnp.dot(h_ref[...], w_ref[...], preferred_element_type=F32)
            if own:
                x_ref, r_ref, o_ref = rest
                o_ref[...] = (x_ref[...].astype(F32) + (v + r_ref[...])).astype(BF16)
            else:
                rest[0][...] = v

        bm = 512
        base = 0 if own else TOK // bm
        col = pl.BlockSpec((bm, B), lambda n, i: (i, n))
        pltpu.emit_pipeline(body, grid=(2, (TOK // 4 if own else TOK) // bm),
                            in_specs=[pl.BlockSpec((bm, HF), lambda n, i: (i + base, 0)), pl.BlockSpec((HF, B), lambda n, i: (0, n))]
                            + ([col, col] if own else []),
                            out_specs=[col])(ha, w2g, *([x, yr] if own else []), y0 if own else yp)

    barrier = pltpu.get_barrier_semaphore()
    friends = [peer, dev(nx, 0), dev(nx, 1), dev(ny, 0), dev(ny, 1)]
    for d in friends:
        pl.semaphore_signal(barrier, inc=1, device_id=(d,), device_id_type=MESH)
    pl.semaphore_wait(barrier, len(friends))

    for d in w1_out(0):
        d.start()
    cx.start()
    cg.start()
    row = pl.BlockSpec((B, D), lambda i: (i, 0))
    pltpu.emit_pipeline(copy_body, grid=(4,),
                        in_specs=[pl.BlockSpec((256, B), lambda i: (0, 2 * i + c)), row],
                        out_specs=[pl.BlockSpec((256, B), lambda i: (me, i)), row])(w1, x, w1g, xa.at[pl.ds(0, TOK)])
    for d in w1_in(0):
        d.wait_recv()
    for d in w1_relay(0):
        d.start()
    for d in w1_out(1):
        d.start()
    pltpu.emit_pipeline(copy_body, grid=(4,),
                        in_specs=[pl.BlockSpec((256, D), lambda i: (i, 0)), row],
                        out_specs=[pl.BlockSpec((256, D), lambda i: (4 * q + i, 0)), row])(w2, g, w2g, ga.at[pl.ds(0, TOK)])
    cx.wait_recv()
    for d in w1_relay_in(0):
        d.wait_recv()
    with jax.named_scope("pa"):
        a_phase()
    cg.wait_recv()

    def at2(i):
        @pl.when(i == 1)
        def _():
            p2[0].start()

        @pl.when(i == 2)
        def _():
            p2[1].start()
            for d in w2_in:
                d.wait_recv()
            for d in w2_relay:
                d.start()

        @pl.when(i == 3)
        def _():
            p2[2].start()

    with jax.named_scope("d2diag"):
        tn(4, ha, ga, s2.at[pl.ds(0, 4)], B, B, first, lambda i: i % 2, half, at=at2)
    p2[3].start()
    with jax.named_scope("e3"):
        e_phase(0, 3)
    p2[0].wait_recv()
    p2[1].wait_recv()
    with jax.named_scope("d2add"):
        tn(2, ha, ga, s2.at[pl.ds(4, 2)], B, B, last, other, half, [(r2, lambda i: 1 - i)])
    p2[4].start()
    p2[5].start()
    for d in w2_relay_in:
        d.wait_recv()
    with jax.named_scope("e1"):
        e_phase(3, 1)

    def at1(i):
        @pl.when(i == 1)
        def _():
            p1d[0].start()

        @pl.when(i == 2)
        def _():
            p1d[1].start()

        @pl.when(i == 3)
        def _():
            for d in p1[0]:
                d.start()

    with jax.named_scope("d1diag"):
        tn(4, xa, da, s1.at[pl.ds(0, 4)], 512, D, first, lambda i: i % 2, half1, at=at1)
    for d in p1[1]:
        d.start()
    with jax.named_scope("ypeer"):
        y_phase(False)
    cy.start()
    p1d[0].wait_recv()
    p1d[1].wait_recv()

    def at1s(i):
        for k in (2, 3):
            @pl.when(i == k - 1)
            def _():
                for d in p1[k]:
                    d.start()

    with jax.named_scope("d1add"):
        tn(4, xa, da, s1.at[pl.ds(4, 4)], 512, D, last, other, half1, [(r1, lambda i: jnp.where(i == 0, 1, 0))], at=at1s)
    co.start()
    for k in range(2, 6):
        p2[k].wait_recv()
    with jax.named_scope("d2own"):
        tn(2, ha, ga, dw2, B, B, lambda i: q, lambda i: i, pl.BlockSpec((B, B), lambda i, k: (0, i)),
           [(r2, lambda i: 2 + i), (r2, lambda i: 5 - i)])
    cy.wait_recv()
    with jax.named_scope("yown"):
        y_phase(True)
    co.wait_recv()
    for pair in p1_in:
        for d in pair:
            d.wait_recv()
    for d in [cx, cg, co, cy] + w2_out + w2_relay + p2 + p1d + [d for pair in p1 for d in pair]:
        d.wait_send()

    @pl.loop(0, 4)
    def _(j):
        for d in w1_out(j) + w1_relay(j):
            d.wait_send()


def _finish(c_ref, ha, hb, hc, w2, xa, xb, xc, ra, rb, rc, y0, dw2, o1, o1r, fa, fb, y_out, dw1_out, dw2_out):
    h = jnp.concatenate([ha[0], hb[0], hc[0]], axis=0)
    m = ha.shape[1]
    for n in range(2):
        s = slice(n * B, (n + 1) * B)
        v = jnp.dot(h, w2[:, s], preferred_element_type=F32)
        for i, (x, r) in enumerate(((xa, ra), (xb, rb), (xc, rc))):
            y_out[i + 1, :, s] = (x[0, :, s].astype(F32) + (v[i * m:(i + 1) * m] + r[0, :, s])).astype(BF16)
    y_out[0] = y0[...]
    dw2_out[...] = dw2[...]
    own = jnp.where(pl.program_id(0) < 4, o1[0], o1r[0])
    dw1_out[...] = own + (fa[0, 0] + fb[0, 0])


def solution(mesh):
    spec = P(None, AX, None)

    def body(x, g, w1, w2):
        c = lax.axis_index(AX) % 2
        shape = lambda s, t: jax.ShapeDtypeStruct(s, t)
        dma = lambda *s: pltpu.SemaphoreType.DMA(s)
        hbm = pl.BlockSpec(memory_space=pl.ANY)
        x = x.reshape(TOK, D)
        outs = [
            shape((T, HF), BF16), shape((HF, D), BF16), shape((TOK, D), F32), shape((TOK // 4, D), BF16), shape((B, D), F32),
            shape((8, 512, D), F32), shape((2, 256, D), F32), shape((4, 2, 256, D), F32),
            shape((T, D), BF16), shape((T, D), BF16), shape((D, HF), BF16), shape((T, HF), BF16), shape((T, HF), BF16),
            shape((6, B, B), F32), shape((6, B, B), F32), shape((2, 512, D), F32), shape((TOK, D), F32),
        ]
        res = pl.pallas_call(
            _kernel,
            out_shape=outs,
            in_specs=[hbm] * 4,
            out_specs=[hbm] * len(outs),
            scratch_shapes=[dma(2), dma(2), dma(4, 7), dma(4, 7), dma(4), dma(4), dma(6), dma(6), dma(6, 2), dma(6, 2),
                            dma(1), dma(1), dma(1), dma(1)],
            compiler_params=pltpu.CompilerParams(collective_id=0, has_side_effects=True, vmem_limit_bytes=VMEM),
            name="step",
        )(x, g.reshape(TOK, D), w1[0], w2[0])
        h, w2g, yr, y0, dw2, s1, o1r, r1f = res[:8]
        part = lambda s, c: (s // 4) * (1 - c[0]) + (1 - s // 4) * c[0]
        n, t = (lambda s: (s // 2) % 2), (lambda s: s % 2)
        mine = lambda s: jnp.minimum(s, 3)
        theirs = lambda s: jnp.maximum(s, 4)
        bm = TOK // 32
        row = lambda m, w=D: pl.BlockSpec((m, w), lambda s, c: (s, 0))
        quarters = lambda w: [pl.BlockSpec((1, bm, w), functools.partial(lambda i, s, c: (i, s, 0), i)) for i in (1, 2, 3)]
        h, x, yr = h.reshape(8, TOK // 4, HF), x.reshape(4, TOK // 4, D), yr.reshape(4, TOK // 4, D)
        y, dw1, dw2 = pl.pallas_call(
            _finish,
            grid_spec=pltpu.PrefetchScalarGridSpec(
                num_scalar_prefetch=1,
                grid=(8,),
                in_specs=quarters(HF) + [pl.BlockSpec((HF, D), lambda s, c: (0, 0), pipeline_mode=pl.Buffered(1))]
                + quarters(D) + quarters(D) + [
                    row(bm), row(B // 8),
                    pl.BlockSpec((1, 256, B), lambda s, c: (6 + n(mine(s)), c[0], t(mine(s)))),
                    pl.BlockSpec((1, 256, B), lambda s, c: (n(theirs(s)), 0, t(theirs(s)))),
                    pl.BlockSpec((1, 1, 256, B), lambda s, c: (n(s), part(s, c), 0, t(s))),
                    pl.BlockSpec((1, 1, 256, B), lambda s, c: (3 - n(s), part(s, c), 0, t(s))),
                ],
                out_specs=[pl.BlockSpec((4, bm, D), lambda s, c: (0, s, 0)), pl.BlockSpec((256, B), lambda s, c: (0, 2 * (2 * n(s) + t(s)) + part(s, c))), row(B // 8)],
            ),
            out_shape=[shape((4, TOK // 4, D), BF16), shape((256, 8192), F32), shape((B, D), F32)],
            compiler_params=pltpu.CompilerParams(dimension_semantics=("arbitrary",), vmem_limit_bytes=VMEM),
            name="finish",
        )(c[None], h, h, h, w2g, x, x, x, yr, yr, yr, y0, dw2, s1, o1r, r1f, r1f)
        return y.reshape(2, TOK // 2, D), dw1[None], dw2[None]

    return jax.shard_map(body, mesh=mesh, in_specs=(spec, spec, spec, spec),
                         out_specs=(spec, spec, spec), check_vma=False)
```
